32 devices in a mesh: seq: 8 (over z, x), grp: 4 (over y, core).
Axes of the slice: x: 2, y: 2, z: 4, core: 2. Of those that a mesh axis runs over, the one named last changes fastest.
Arguments:
- delta_codes: int32 [16, 16, 2048, 128], P('grp', None, 'seq'), may hold values from -63 to 63, as said below
- scale_index: int32 [16, 16, 128], P('grp', None, 'seq'), may hold values from 0 to 15
- anchor_codes: int32 [16, 16, 128], P('grp'), may hold values from -8 to 7
- scale_table: float32 [16, 128], replicated, may hold values from 5e-05 to 0.0005
- anchor_scale: float32 [128], replicated, may hold values from 0.0001 to 0.001
Outputs:
- decode_cache: bfloat16 [4, 64, 2048, 128], P('grp', 'seq')
The draws below stay inside these ranges and needn't reach their ends.
Inputs may be any that keep to these rules, and one draw needn't show every extreme that they name: `delta_codes`: for every sequence, head and channel, the running sum of the codes from the sequence's first token lies in -32 .. 31 after every token, and in -2 .. 1 after the last token of each group of 16 tokens.
All inputs are finite; a program needn't handle non-finite values.
Results may differ from the reference program's by a relative error of at most 0.001.
Values may be sent and summed in bfloat16 or wider, within the bound.
A program may use at most 128 MiB of HBM per device.

```python
import math
import jax
import jax.numpy as jnp
from jax import lax

HEAD_DIM = 128
KV_HEADS = 16
GROUP_LEN = 16
LEVELS = 16
SEQS = 16
LENGTH = 2048
N_GRP = 4


def draw_delta_codes(key, part):
    running_key = jax.random.fold_in(key, 11)
    running = jax.random.randint(running_key, (SEQS, KV_HEADS, LENGTH, HEAD_DIM), -32, 32, dtype=jnp.int32)
    position = lax.broadcasted_iota(jnp.int32, (1, 1, LENGTH, 1), 2)
    group_end = position % GROUP_LEN == GROUP_LEN - 1
    running = jnp.where(group_end, jnp.remainder(running, 4) - 2, running)
    earlier = jnp.pad(running[:, :, :-1, :], ((0, 0), (0, 0), (1, 0), (0, 0)))
    return running - earlier


def plant(values, key, low, largest):
    dims = values.shape
    place = [jax.random.randint(jax.random.fold_in(key, axis), (), 0, dims[axis]) for axis in range(len(dims))]
    values = values.at[tuple(place)].set(low)
    longest = dims.index(max(dims))
    place[longest] = (place[longest] + 1) % dims[longest]
    return values.at[tuple(place)].set(largest)


def setup_inputs(seed: int = 0) -> dict:
    seeds = jax.random.split(jax.random.key(seed), 6)
    delta_codes = draw_delta_codes(jax.random.fold_in(seeds[5], 71), 0)
    scale_index = plant(jax.random.randint(seeds[1], (SEQS, KV_HEADS, LENGTH // GROUP_LEN), 0, LEVELS), jax.random.fold_in(seeds[1], 1), 0, LEVELS - 1).astype(jnp.int32)
    anchor_codes = plant(jax.random.randint(seeds[2], (SEQS, KV_HEADS, HEAD_DIM), -8, 8), jax.random.fold_in(seeds[2], 1), -8, 7).astype(jnp.int32)
    scale_table = jnp.clip(jnp.exp(jax.random.uniform(seeds[3], (LEVELS, HEAD_DIM), jnp.float32, math.log(4.999999873689376e-05), math.log(0.0005))), 4.999999873689376e-05, 0.0005)
    anchor_scale = jnp.clip(jnp.exp(jax.random.uniform(seeds[4], (HEAD_DIM,), jnp.float32, math.log(0.0001), math.log(0.001))), 0.0001, 0.001)
    return {"delta_codes": delta_codes, "scale_index": scale_index, "anchor_codes": anchor_codes, "scale_table": scale_table, "anchor_scale": anchor_scale}


def reference(delta_codes, scale_index, anchor_codes, scale_table, anchor_scale):
    def one_sequence(items):
        code_vals, scale_ids, anchors = items
        scales = scale_table[scale_ids]
        shaped = code_vals.astype(jnp.float32).reshape(KV_HEADS, LENGTH // GROUP_LEN, GROUP_LEN, HEAD_DIM)
        deltas = shaped * scales[:, :, None, :]
        summed = jnp.cumsum(deltas.reshape(KV_HEADS, LENGTH, HEAD_DIM), axis=1)
        anchor_vals = anchors.astype(jnp.float32) * anchor_scale
        return (summed + anchor_vals[:, None, :]).astype(jnp.bfloat16)

    rebuilt = lax.map(one_sequence, (delta_codes, scale_index, anchor_codes))
    arranged = rebuilt.reshape(SEQS, N_GRP, KV_HEADS // N_GRP, LENGTH, HEAD_DIM).transpose(1, 0, 2, 3, 4)
    return arranged.reshape(N_GRP, SEQS * (KV_HEADS // N_GRP), LENGTH, HEAD_DIM)
```

```python
import functools

import jax
import jax.numpy as jnp
from jax import lax
from jax.experimental import pallas as pl
from jax.experimental.pallas import tpu as pltpu
from jax.sharding import PartitionSpec as P

MESH = pl.DeviceIdType.MESH
HIGHEST = lax.Precision.HIGHEST


def exchange(
    codes, index_ref, anchor_ref, table_ref, anchor_scale_ref,
    landed, scales_ref, base_ref,
    raw, sums, index_out, index_in, anchor_out, anchor_in,
    load_sem, send_sem, recv_sem, isend_sem, irecv_sem, asend_sem, arecv_sem,
):
    seqs, grps = lax.axis_size("seq"), lax.axis_size("grp")
    s, g = lax.axis_index("seq"), lax.axis_index("grp")
    blocks, rows, tokens, channels = sums.shape
    heads = codes.shape[1] // grps
    per_grp = blocks // grps
    seq_rows, head_rows = max(1, rows // heads), min(rows, heads)
    levels = table_ref.shape[0]
    groups = index_ref.shape[2]
    group_len = tokens // groups

    def place(d):
        h = lax.rem(g + d // per_grp, grps)
        i = lax.rem(s + d, per_grp)
        first = i * rows
        return h, g * per_grp + i, first // heads, h * heads + lax.rem(first, heads)

    def is_me(d):
        h, to_s, _, _ = place(d)
        return jnp.logical_and(h == g, to_s == s)

    def load(d):
        _, _, b0, k0 = place(d)
        return pltpu.make_async_copy(
            codes.at[pl.ds(b0, seq_rows), pl.ds(k0, head_rows)], raw.at[d], load_sem.at[d]
        )

    def remote(src, dst, ssem, rsem, d):
        h, to_s, _, _ = place(d)
        return pltpu.make_async_remote_copy(
            src_ref=src, dst_ref=dst, send_sem=ssem, recv_sem=rsem,
            device_id={"seq": to_s, "grp": h}, device_id_type=MESH,
        )

    def window(j):
        return landed.at[:, pl.ds(pl.multiple_of(j * tokens, tokens), tokens), :]

    def send_sums(d):
        return remote(sums.at[d], window(s), send_sem.at[d], recv_sem.at[s], d)

    def send_index(d):
        return remote(index_out.at[d], index_in.at[s], isend_sem.at[d], irecv_sem.at[s], d)

    def send_anchor(d):
        return remote(anchor_out.at[d], anchor_in, asend_sem.at[d], arecv_sem, d)

    @pl.loop(0, blocks)
    def _(d):
        load(d).start()

    barrier = pltpu.get_barrier_semaphore()
    from_g = s // per_grp

    @pl.loop(0, seqs)
    def _(j):
        @pl.when(jnp.logical_not(jnp.logical_and(j == s, from_g == g)))
        def _():
            pl.semaphore_signal(
                barrier, inc=1, device_id={"seq": j, "grp": from_g}, device_id_type=MESH
            )

    kept = jnp.where(from_g == g, 1, 0)

    for d in range(blocks):
        _, _, b0, k0 = place(d)
        for b in range(seq_rows):
            part = pl.ds(b * head_rows, head_rows)
            index_out[d, part, :] = index_ref[b0 + b, pl.ds(k0, head_rows), :]
            anchor_out[d, part, :] = anchor_ref[b0 + b, pl.ds(k0, head_rows), :]

    t_out = lax.broadcasted_iota(jnp.int32, (tokens, tokens), 0)
    t_in = lax.broadcasted_iota(jnp.int32, (tokens, tokens), 1)
    same = t_out // group_len == t_in // group_len
    within = jnp.where(jnp.logical_and(same, t_out >= t_in), 1.0, 0.0).astype(jnp.bfloat16)

    @pl.loop(0, blocks)
    def _(d):
        load(d).wait()
        for r in range(rows):
            x = raw[d, r // head_rows, r % head_rows].astype(jnp.float32).astype(jnp.bfloat16)
            run = jnp.dot(within, x, preferred_element_type=jnp.float32)
            sums[d, r] = run.astype(jnp.bfloat16)

        @pl.when(d == 0)
        def _():
            pl.semaphore_wait(barrier, blocks - kept)

        @pl.when(jnp.logical_not(is_me(d)))
        def _():
            send_index(d).start()

            @pl.when(s == 0)
            def _():
                send_anchor(d).start()

            send_sums(d).start()

    @pl.loop(0, blocks)
    def _(d):
        @pl.when(is_me(d))
        def _():
            index_in[s] = index_out[d]
            for r in range(rows):
                landed[r, pl.ds(pl.multiple_of(s * tokens, tokens), tokens), :] = sums[d, r]

            @pl.when(s == 0)
            def _():
                anchor_in[...] = anchor_out[d]

    mine = jnp.logical_and(from_g == g, s == 0)

    @pl.when(jnp.logical_not(mine))
    def _():
        send_anchor(0).wait_recv()

    for r in range(rows):
        base_ref[r] = anchor_in[pl.ds(r, 1), :].astype(jnp.float32) * anchor_scale_ref[...]

    def from_me(j):
        return jnp.logical_and(j == s, from_g == g)

    @pl.loop(0, seqs)
    def _(j):
        @pl.when(jnp.logical_not(from_me(j)))
        def _():
            remote(index_out.at[0], index_in.at[j], isend_sem.at[0], irecv_sem.at[j], 0).wait_recv()

        table = table_ref[...]
        for r in range(rows):
            ids = jnp.broadcast_to(index_in[j, pl.ds(r, 1), :], (levels, groups))
            hot = (ids == lax.broadcasted_iota(jnp.int32, (levels, groups), 0)).astype(jnp.float32)
            found = lax.dot_general(
                hot, table, (((0,), (0,)), ((), ())),
                precision=HIGHEST, preferred_element_type=jnp.float32,
            )
            scales_ref[r, pl.ds(pl.multiple_of(j * groups, groups), groups), :] = found

    @pl.loop(0, seqs)
    def _(j):
        @pl.when(jnp.logical_not(from_me(j)))
        def _():
            remote(sums.at[0], window(j), send_sem.at[0], recv_sem.at[j], 0).wait_recv()

    @pl.loop(0, blocks)
    def _(d):
        @pl.when(jnp.logical_not(is_me(d)))
        def _():
            send_index(d).wait_send()

            @pl.when(s == 0)
            def _():
                send_anchor(d).wait_send()

            send_sums(d).wait_send()


def rebuild(sums_ref, scales_ref, base_ref, out_ref, carry):
    r, c = pl.program_id(0), pl.program_id(1)
    step, channels = out_ref.shape[2:]
    group_len = sums_ref.shape[1] // scales_ref.shape[1]
    groups = step // group_len

    @pl.when(c == 0)
    def _():
        carry[...] = base_ref[r]

    x = sums_ref[r, pl.ds(pl.multiple_of(c * step, step), step), :]
    x = x.astype(jnp.float32).reshape(groups, group_len, channels)
    scale = scales_ref[r, pl.ds(pl.multiple_of(c * groups, groups), groups), :]
    total = x[:, group_len - 1, :] * scale
    row = lax.broadcasted_iota(jnp.int32, (groups, groups), 0)
    col = lax.broadcasted_iota(jnp.int32, (groups, groups), 1)
    earlier = (row > col).astype(jnp.float32)
    base = jnp.dot(
        earlier, total, precision=HIGHEST, preferred_element_type=jnp.float32
    ) + carry[...]
    carry[...] = base[groups - 1:] + total[groups - 1:]
    out = x * scale[:, None, :] + base[:, None, :]
    out_ref[0, 0] = out.reshape(groups * group_len, channels).astype(jnp.bfloat16)


def on_device(delta_codes, scale_index, anchor_codes, scale_table, anchor_scale):
    seqs, grps = lax.axis_size("seq"), lax.axis_size("grp")
    seq_local, kv_heads, tokens, channels = delta_codes.shape
    groups = scale_index.shape[2]
    heads = kv_heads // grps
    rows = seq_local * grps * heads // seqs
    blocks = seq_local * kv_heads // rows
    seq_rows, head_rows = max(1, rows // heads), min(rows, heads)
    length = seqs * tokens
    vmem = pl.BlockSpec(memory_space=pltpu.VMEM)
    hbm = pl.BlockSpec(memory_space=pltpu.HBM)
    sums, scales, base = pl.pallas_call(
        exchange,
        out_shape=(
            jax.ShapeDtypeStruct((rows, length, channels), jnp.bfloat16),
            jax.ShapeDtypeStruct((rows, seqs * groups, channels), jnp.float32),
            jax.ShapeDtypeStruct((rows, 1, channels), jnp.float32),
        ),
        in_specs=[hbm, vmem, vmem, vmem, vmem],
        out_specs=(vmem, vmem, vmem),
        scratch_shapes=[
            pltpu.VMEM((blocks, seq_rows, head_rows, tokens, channels), jnp.int32),
            pltpu.VMEM((blocks, rows, tokens, channels), jnp.bfloat16),
            pltpu.VMEM((blocks, rows, groups), jnp.int32),
            pltpu.VMEM((seqs, rows, groups), jnp.int32),
            pltpu.VMEM((blocks, rows, channels), jnp.int32),
            pltpu.VMEM((rows, channels), jnp.int32),
            pltpu.SemaphoreType.DMA((blocks,)),
            pltpu.SemaphoreType.DMA((blocks,)),
            pltpu.SemaphoreType.DMA((seqs,)),
            pltpu.SemaphoreType.DMA((blocks,)),
            pltpu.SemaphoreType.DMA((seqs,)),
            pltpu.SemaphoreType.DMA((blocks,)),
            pltpu.SemaphoreType.DMA,
        ],
        compiler_params=pltpu.CompilerParams(
            collective_id=0, has_side_effects=True, vmem_limit_bytes=56 * 1024 * 1024
        ),
        name="exchange",
    )(delta_codes, scale_index, anchor_codes, scale_table, anchor_scale[None])

    step = 4 * tokens
    out = pl.pallas_call(
        rebuild,
        grid=(rows, length // step),
        out_shape=jax.ShapeDtypeStruct((1, rows, length, channels), jnp.bfloat16),
        in_specs=[vmem, vmem, vmem],
        out_specs=pl.BlockSpec((1, 1, step, channels), lambda r, c: (0, r, c, 0)),
        scratch_shapes=[pltpu.VMEM((1, channels), jnp.float32)],
        compiler_params=pltpu.CompilerParams(vmem_limit_bytes=16 * 1024 * 1024),
        name="rebuild",
    )(sums, scales, base)
    return out


def solution(mesh):
    placed = (P("grp", None, "seq", None), P("grp", None, "seq"), P("grp", None, None), P(), P())
    return jax.shard_map(
        on_device,
        mesh=mesh,
        in_specs=placed,
        out_specs=P("grp", "seq", None, None),
        check_vma=False,
    )
```

```python
import functools

import jax
import jax.numpy as jnp
from jax import lax
from jax.experimental import pallas as pl
from jax.experimental.pallas import tpu as pltpu
from jax.sharding import PartitionSpec as P

MESH = pl.DeviceIdType.MESH
CHUNKS = 4
HIGHEST = lax.Precision.HIGHEST


def exchange(
    codes, index_ref, anchor_ref, table_ref, anchor_scale_ref,
    landed, scales_ref, base_ref,
    raw, sums, relay, index_out, index_in, anchor_out, anchor_in,
    load_sem, send_sem, recv_sem, isend_sem, irecv_sem, asend_sem, arecv_sem,
    relay_sem, forward_sem,
):
    seqs, grps = lax.axis_size("seq"), lax.axis_size("grp")
    s, g = lax.axis_index("seq"), lax.axis_index("grp")
    blocks, rows, tokens, channels = sums.shape
    heads = codes.shape[1] // grps
    per_grp = blocks // grps
    half = grps // 2
    partner = lax.rem(g + half, grps)
    chunks = relay.shape[1]
    chunk_rows = rows // chunks
    passed = blocks // 2 * chunks
    seq_rows, head_rows = max(1, rows // heads), min(rows, heads)
    levels = table_ref.shape[0]
    groups = index_ref.shape[2]
    group_len = tokens // groups

    def place_from(d, own):
        e = d // 2
        side = lax.rem(own // half + 1 + d, 2)
        h = side * half + lax.rem(own + e // per_grp, half)
        i = lax.rem(s + e, per_grp)
        first = i * rows
        return h, own * per_grp + i, first // heads, h * heads + lax.rem(first, heads)

    def place(d):
        return place_from(d, g)

    def is_me(d):
        h, to_s, _, _ = place(d)
        return jnp.logical_and(h == g, to_s == s)

    def load(d):
        _, _, b0, k0 = place(d)
        return pltpu.make_async_copy(
            codes.at[pl.ds(b0, seq_rows), pl.ds(k0, head_rows)], raw.at[d], load_sem.at[d]
        )

    def remote(src, dst, ssem, rsem, d):
        h, to_s, _, _ = place(d)
        return pltpu.make_async_remote_copy(
            src_ref=src, dst_ref=dst, send_sem=ssem, recv_sem=rsem,
            device_id={"seq": to_s, "grp": h}, device_id_type=MESH,
        )

    def window(j):
        return landed.at[:, pl.ds(pl.multiple_of(j * tokens, tokens), tokens), :]

    def send_sums(d):
        return remote(sums.at[d], window(s), send_sem.at[d], recv_sem.at[s], d)

    def at_partner(d):
        h, to_s, _, _ = place(d)
        return jnp.logical_and(h == partner, to_s == s)

    def send_relay(e, c):
        return pltpu.make_async_remote_copy(
            src_ref=sums.at[2 * e, pl.ds(c * chunk_rows, chunk_rows)], dst_ref=relay.at[e, c],
            send_sem=send_sem.at[2 * e], recv_sem=relay_sem.at[e, c],
            device_id={"seq": s, "grp": partner}, device_id_type=MESH,
        )

    def relayed(e):
        h, to_s, _, _ = place_from(2 * e, partner)
        return jnp.logical_not(jnp.logical_and(h == g, to_s == s))

    def forward(e, c):
        h, to_s, _, _ = place_from(2 * e, partner)
        span = pl.ds(pl.multiple_of(s * tokens, tokens), tokens)
        return pltpu.make_async_remote_copy(
            src_ref=relay.at[e, c], dst_ref=landed.at[pl.ds(c * chunk_rows, chunk_rows), span, :],
            send_sem=forward_sem.at[e], recv_sem=recv_sem.at[s],
            device_id={"seq": to_s, "grp": h}, device_id_type=MESH,
        )

    def pass_on(n):
        e, c = n // chunks, lax.rem(n, chunks)

        @pl.when(relayed(e))
        def _():
            send_relay(e, c).wait_recv()
            forward(e, c).start()

    def send_index(d):
        return remote(index_out.at[d], index_in.at[s], isend_sem.at[d], irecv_sem.at[s], d)

    def send_anchor(d):
        return remote(anchor_out.at[d], anchor_in, asend_sem.at[d], arecv_sem, d)

    @pl.loop(0, blocks)
    def _(d):
        load(d).start()

    barrier = pltpu.get_barrier_semaphore()
    from_g = s // per_grp

    inside = lax.rem(from_g, half) == lax.rem(g, half)

    @pl.loop(0, 2 * seqs)
    def _(n):
        j = n // 2
        to_g = lax.rem(from_g + lax.rem(n, 2) * half, grps)

        @pl.when(jnp.logical_not(jnp.logical_and(j == s, to_g == g)))
        def _():
            pl.semaphore_signal(
                barrier, inc=1, device_id={"seq": j, "grp": to_g}, device_id_type=MESH
            )

    @pl.when(jnp.logical_not(inside))
    def _():
        pl.semaphore_signal(
            barrier, inc=1, device_id={"seq": s, "grp": partner}, device_id_type=MESH
        )

    expected = 2 * blocks + jnp.where(inside, -1, 1)

    for d in range(blocks):
        _, _, b0, k0 = place(d)
        for b in range(seq_rows):
            part = pl.ds(b * head_rows, head_rows)
            index_out[d, part, :] = index_ref[b0 + b, pl.ds(k0, head_rows), :]
            anchor_out[d, part, :] = anchor_ref[b0 + b, pl.ds(k0, head_rows), :]

    t_out = lax.broadcasted_iota(jnp.int32, (tokens, tokens), 0)
    t_in = lax.broadcasted_iota(jnp.int32, (tokens, tokens), 1)
    same = t_out // group_len == t_in // group_len
    within = jnp.where(jnp.logical_and(same, t_out >= t_in), 1.0, 0.0).astype(jnp.bfloat16)

    @pl.loop(0, blocks)
    def _(d):
        load(d).wait()
        for r in range(rows):
            x = raw[d, r // head_rows, r % head_rows].astype(jnp.float32).astype(jnp.bfloat16)
            run = jnp.dot(within, x, preferred_element_type=jnp.float32)
            sums[d, r] = run.astype(jnp.bfloat16)

        @pl.when(d == 0)
        def _():
            pl.semaphore_wait(barrier, expected)

        @pl.when(jnp.logical_not(is_me(d)))
        def _():
            send_index(d).start()

            @pl.when(s == 0)
            def _():
                send_anchor(d).start()

            via = jnp.logical_and(lax.rem(d, 2) == 0, jnp.logical_not(at_partner(d)))

            @pl.when(via)
            def _():
                for c in range(chunks):
                    send_relay(d // 2, c).start()

            @pl.when(jnp.logical_not(via))
            def _():
                send_sums(d).start()

        @pl.when(jnp.logical_and(d >= 2, d - 2 < passed))
        def _():
            pass_on(d - 2)

    @pl.loop(min(blocks - 2, passed), passed)
    def _(n):
        pass_on(n)

    @pl.loop(0, blocks)
    def _(d):
        @pl.when(is_me(d))
        def _():
            index_in[s] = index_out[d]
            for r in range(rows):
                landed[r, pl.ds(pl.multiple_of(s * tokens, tokens), tokens), :] = sums[d, r]

            @pl.when(s == 0)
            def _():
                anchor_in[...] = anchor_out[d]

    mine = jnp.logical_and(from_g == g, s == 0)

    @pl.when(jnp.logical_not(mine))
    def _():
        send_anchor(0).wait_recv()

    for r in range(rows):
        base_ref[r] = anchor_in[pl.ds(r, 1), :].astype(jnp.float32) * anchor_scale_ref[...]

    def from_me(j):
        return jnp.logical_and(j == s, from_g == g)

    @pl.loop(0, seqs)
    def _(j):
        @pl.when(jnp.logical_not(from_me(j)))
        def _():
            remote(index_out.at[0], index_in.at[j], isend_sem.at[0], irecv_sem.at[j], 0).wait_recv()

        table = table_ref[...]
        for r in range(rows):
            ids = jnp.broadcast_to(index_in[j, pl.ds(r, 1), :], (levels, groups))
            hot = (ids == lax.broadcasted_iota(jnp.int32, (levels, groups), 0)).astype(jnp.float32)
            found = lax.dot_general(
                hot, table, (((0,), (0,)), ((), ())),
                precision=HIGHEST, preferred_element_type=jnp.float32,
            )
            scales_ref[r, pl.ds(pl.multiple_of(j * groups, groups), groups), :] = found

    @pl.loop(0, seqs)
    def _(j):
        @pl.when(jnp.logical_not(from_me(j)))
        def _():
            remote(sums.at[0], window(j), send_sem.at[0], recv_sem.at[j], 0).wait_recv()

    @pl.loop(0, blocks)
    def _(d):
        @pl.when(jnp.logical_not(is_me(d)))
        def _():
            send_index(d).wait_send()

            @pl.when(s == 0)
            def _():
                send_anchor(d).wait_send()

            send_sums(d).wait_send()

    @pl.loop(0, blocks // 2)
    def _(e):
        @pl.when(relayed(e))
        def _():
            for c in range(chunks):
                forward(e, c).wait_send()


def rebuild(sums_ref, scales_ref, base_ref, out_ref, carry):
    r, c = pl.program_id(0), pl.program_id(1)
    step, channels = out_ref.shape[2:]
    group_len = sums_ref.shape[1] // scales_ref.shape[1]
    groups = step // group_len

    @pl.when(c == 0)
    def _():
        carry[...] = base_ref[r]

    x = sums_ref[r, pl.ds(pl.multiple_of(c * step, step), step), :]
    x = x.astype(jnp.float32).reshape(groups, group_len, channels)
    scale = scales_ref[r, pl.ds(pl.multiple_of(c * groups, groups), groups), :]
    total = x[:, group_len - 1, :] * scale
    row = lax.broadcasted_iota(jnp.int32, (groups, groups), 0)
    col = lax.broadcasted_iota(jnp.int32, (groups, groups), 1)
    earlier = (row > col).astype(jnp.float32)
    base = jnp.dot(
        earlier, total, precision=HIGHEST, preferred_element_type=jnp.float32
    ) + carry[...]
    carry[...] = base[groups - 1:] + total[groups - 1:]
    out = x * scale[:, None, :] + base[:, None, :]
    out_ref[0, 0] = out.reshape(groups * group_len, channels).astype(jnp.bfloat16)


def on_device(delta_codes, scale_index, anchor_codes, scale_table, anchor_scale):
    seqs, grps = lax.axis_size("seq"), lax.axis_size("grp")
    seq_local, kv_heads, tokens, channels = delta_codes.shape
    groups = scale_index.shape[2]
    heads = kv_heads // grps
    rows = seq_local * grps * heads // seqs
    blocks = seq_local * kv_heads // rows
    seq_rows, head_rows = max(1, rows // heads), min(rows, heads)
    chunks = min(rows, CHUNKS)
    length = seqs * tokens
    vmem = pl.BlockSpec(memory_space=pltpu.VMEM)
    hbm = pl.BlockSpec(memory_space=pltpu.HBM)
    sums, scales, base = pl.pallas_call(
        exchange,
        out_shape=(
            jax.ShapeDtypeStruct((rows, length, channels), jnp.bfloat16),
            jax.ShapeDtypeStruct((rows, seqs * groups, channels), jnp.float32),
            jax.ShapeDtypeStruct((rows, 1, channels), jnp.float32),
        ),
        in_specs=[hbm, vmem, vmem, vmem, vmem],
        out_specs=(vmem, vmem, vmem),
        scratch_shapes=[
            pltpu.VMEM((blocks, seq_rows, head_rows, tokens, channels), jnp.int32),
            pltpu.VMEM((blocks, rows, tokens, channels), jnp.bfloat16),
            pltpu.VMEM((blocks // 2, chunks, rows // chunks, tokens, channels), jnp.bfloat16),
            pltpu.VMEM((blocks, rows, groups), jnp.int32),
            pltpu.VMEM((seqs, rows, groups), jnp.int32),
            pltpu.VMEM((blocks, rows, channels), jnp.int32),
            pltpu.VMEM((rows, channels), jnp.int32),
            pltpu.SemaphoreType.DMA((blocks,)),
            pltpu.SemaphoreType.DMA((blocks,)),
            pltpu.SemaphoreType.DMA((seqs,)),
            pltpu.SemaphoreType.DMA((blocks,)),
            pltpu.SemaphoreType.DMA((seqs,)),
            pltpu.SemaphoreType.DMA((blocks,)),
            pltpu.SemaphoreType.DMA,
            pltpu.SemaphoreType.DMA((blocks // 2, chunks)),
            pltpu.SemaphoreType.DMA((blocks // 2,)),
        ],
        compiler_params=pltpu.CompilerParams(
            collective_id=0, has_side_effects=True, vmem_limit_bytes=48 * 1024 * 1024
        ),
        name="exchange",
    )(delta_codes, scale_index, anchor_codes, scale_table, anchor_scale[None])

    step = 4 * tokens
    out = pl.pallas_call(
        rebuild,
        grid=(rows, length // step),
        out_shape=jax.ShapeDtypeStruct((1, rows, length, channels), jnp.bfloat16),
        in_specs=[vmem, vmem, vmem],
        out_specs=pl.BlockSpec((1, 1, step, channels), lambda r, c: (0, r, c, 0)),
        scratch_shapes=[pltpu.VMEM((1, channels), jnp.float32)],
        compiler_params=pltpu.CompilerParams(vmem_limit_bytes=16 * 1024 * 1024),
        name="rebuild",
    )(sums, scales, base)
    return out


def solution(mesh):
    placed = (P("grp", None, "seq", None), P("grp", None, "seq"), P("grp", None, None), P(), P())
    return jax.shard_map(
        on_device,
        mesh=mesh,
        in_specs=placed,
        out_specs=P("grp", "seq", None, None),
        check_vma=False,
    )
```

```python
import functools

import jax
import jax.numpy as jnp
from jax import lax
from jax.experimental import pallas as pl
from jax.experimental.pallas import tpu as pltpu
from jax.sharding import PartitionSpec as P

MESH = pl.DeviceIdType.MESH
CHUNKS = 4
LAG = 1
HIGHEST = lax.Precision.HIGHEST


def exchange(
    codes, index_hbm, anchor_hbm, table_hbm, anchor_scale_hbm,
    landed, scales_ref, base_ref,
    raw, sums, relay, index_out, index_in, anchor_out, anchor_in,
    load_sem, send_sem, recv_sem, isend_sem, irecv_sem, asend_sem, arecv_sem,
    relay_sem, forward_sem,
    index_ref, anchor_ref, table_ref, anchor_scale_ref, small_sem,
):
    seqs, grps = lax.axis_size("seq"), lax.axis_size("grp")
    s, g = lax.axis_index("seq"), lax.axis_index("grp")
    blocks, rows, tokens, channels = sums.shape
    heads = codes.shape[1] // grps
    per_grp = blocks // grps
    half = grps // 2
    partner = lax.rem(g + half, grps)
    chunks = relay.shape[1]
    chunk_rows = rows // chunks
    passed = blocks // 2 * chunks
    seq_rows, head_rows = max(1, rows // heads), min(rows, heads)
    levels = table_ref.shape[0]
    groups = index_hbm.shape[2]
    group_len = tokens // groups

    def place_from(d, own):
        e = d // 2
        side = lax.rem(own // half + 1 + d, 2)
        h = side * half + lax.rem(own + e // per_grp, half)
        i = lax.rem(s + e, per_grp)
        first = i * rows
        return h, own * per_grp + i, first // heads, h * heads + lax.rem(first, heads)

    def place(d):
        return place_from(d, g)

    def is_me(d):
        h, to_s, _, _ = place(d)
        return jnp.logical_and(h == g, to_s == s)

    def load(d):
        _, _, b0, k0 = place(d)
        return pltpu.make_async_copy(
            codes.at[pl.ds(b0, seq_rows), pl.ds(k0, head_rows)], raw.at[d], load_sem.at[d]
        )

    def remote(src, dst, ssem, rsem, d):
        h, to_s, _, _ = place(d)
        return pltpu.make_async_remote_copy(
            src_ref=src, dst_ref=dst, send_sem=ssem, recv_sem=rsem,
            device_id={"seq": to_s, "grp": h}, device_id_type=MESH,
        )

    def window(j):
        return landed.at[:, pl.ds(pl.multiple_of(j * tokens, tokens), tokens), :]

    def send_sums(d):
        return remote(sums.at[d], window(s), send_sem.at[d], recv_sem.at[s], d)

    def at_partner(d):
        h, to_s, _, _ = place(d)
        return jnp.logical_and(h == partner, to_s == s)

    def part(c):
        return pl.ds(c * chunk_rows, chunk_rows)

    def send_relay(e, c):
        return pltpu.make_async_remote_copy(
            src_ref=sums.at[2 * e, part(c)], dst_ref=relay.at[e, c],
            send_sem=send_sem.at[2 * e], recv_sem=relay_sem.at[e, c],
            device_id={"seq": s, "grp": partner}, device_id_type=MESH,
        )

    def send_part(d, c):
        span = pl.ds(pl.multiple_of(s * tokens, tokens), tokens)
        return remote(
            sums.at[d, part(c)], landed.at[part(c), span, :], send_sem.at[d], recv_sem.at[s], d
        )

    def relayed(e):
        h, to_s, _, _ = place_from(2 * e, partner)
        return jnp.logical_not(jnp.logical_and(h == g, to_s == s))

    def forward(e, c):
        h, to_s, _, _ = place_from(2 * e, partner)
        span = pl.ds(pl.multiple_of(s * tokens, tokens), tokens)
        return pltpu.make_async_remote_copy(
            src_ref=relay.at[e, c], dst_ref=landed.at[pl.ds(c * chunk_rows, chunk_rows), span, :],
            send_sem=forward_sem.at[e], recv_sem=recv_sem.at[s],
            device_id={"seq": to_s, "grp": h}, device_id_type=MESH,
        )

    def pass_on(n):
        e, c = n // chunks, lax.rem(n, chunks)

        @pl.when(relayed(e))
        def _():
            send_relay(e, c).wait_recv()
            forward(e, c).start()

    def send_index(d):
        return remote(index_out.at[d], index_in.at[s], isend_sem.at[d], irecv_sem.at[s], d)

    def send_anchor(d):
        return remote(anchor_out.at[d], anchor_in, asend_sem.at[d], arecv_sem, d)

    ahead = min(2, blocks)
    for d in range(ahead):
        load(d).start()

    small = (
        (index_hbm, index_ref), (anchor_hbm, anchor_ref),
        (table_hbm, table_ref), (anchor_scale_hbm, anchor_scale_ref),
    )
    fetches = [
        pltpu.make_async_copy(src, dst, small_sem.at[n]) for n, (src, dst) in enumerate(small)
    ]
    for fetch in fetches:
        fetch.start()

    barrier = pltpu.get_barrier_semaphore()
    from_g = s // per_grp

    inside = lax.rem(from_g, half) == lax.rem(g, half)

    @pl.loop(0, 2 * seqs)
    def _(n):
        j = n // 2
        to_g = lax.rem(from_g + lax.rem(n, 2) * half, grps)

        @pl.when(jnp.logical_not(jnp.logical_and(j == s, to_g == g)))
        def _():
            pl.semaphore_signal(
                barrier, inc=1, device_id={"seq": j, "grp": to_g}, device_id_type=MESH
            )

    @pl.when(jnp.logical_not(inside))
    def _():
        pl.semaphore_signal(
            barrier, inc=1, device_id={"seq": s, "grp": partner}, device_id_type=MESH
        )

    expected = 2 * blocks + jnp.where(inside, -1, 1)

    t_out = lax.broadcasted_iota(jnp.int32, (tokens, tokens), 0)
    t_in = lax.broadcasted_iota(jnp.int32, (tokens, tokens), 1)
    same = t_out // group_len == t_in // group_len
    within = jnp.where(jnp.logical_and(same, t_out >= t_in), 1.0, 0.0).astype(jnp.bfloat16)

    @pl.loop(0, blocks)
    def _(d):
        load(d).wait()

        @pl.when(d + ahead < blocks)
        def _():
            load(d + ahead).start()

        away = jnp.logical_not(is_me(d))
        via = jnp.logical_and(lax.rem(d, 2) == 0, jnp.logical_not(at_partner(d)))
        straight = jnp.logical_and(away, jnp.logical_not(via))
        for c in range(chunks):
            for r in range(c * chunk_rows, (c + 1) * chunk_rows):
                x = raw[d, r // head_rows, r % head_rows].astype(jnp.float32).astype(jnp.bfloat16)
                run = jnp.dot(within, x, preferred_element_type=jnp.float32)
                sums[d, r] = run.astype(jnp.bfloat16)

            if c == 0:
                @pl.when(d == 0)
                def _():
                    pl.semaphore_wait(barrier, expected)

            @pl.when(via)
            def _():
                send_relay(d // 2, c).start()

            @pl.when(straight)
            def _():
                send_part(d, c).start()

        @pl.when(jnp.logical_and(d >= LAG, d - LAG < passed))
        def _():
            pass_on(d - LAG)

    for fetch in fetches:
        fetch.wait()

    @pl.loop(0, blocks)
    def _(d):
        _, _, b0, k0 = place(d)
        for b in range(seq_rows):
            these = pl.ds(b * head_rows, head_rows)
            index_out[d, these, :] = index_ref[b0 + b, pl.ds(k0, head_rows), :]
            anchor_out[d, these, :] = anchor_ref[b0 + b, pl.ds(k0, head_rows), :]

        @pl.when(jnp.logical_not(is_me(d)))
        def _():
            send_index(d).start()

            @pl.when(s == 0)
            def _():
                send_anchor(d).start()

    @pl.loop(min(blocks - LAG, passed), passed)
    def _(n):
        pass_on(n)

    @pl.loop(0, blocks)
    def _(d):
        @pl.when(is_me(d))
        def _():
            index_in[s] = index_out[d]
            for r in range(rows):
                landed[r, pl.ds(pl.multiple_of(s * tokens, tokens), tokens), :] = sums[d, r]

            @pl.when(s == 0)
            def _():
                anchor_in[...] = anchor_out[d]

    mine = jnp.logical_and(from_g == g, s == 0)

    @pl.when(jnp.logical_not(mine))
    def _():
        send_anchor(0).wait_recv()

    for r in range(rows):
        base_ref[r] = anchor_in[pl.ds(r, 1), :].astype(jnp.float32) * anchor_scale_ref[...]

    def from_me(j):
        return jnp.logical_and(j == s, from_g == g)

    @pl.loop(0, seqs)
    def _(j):
        @pl.when(jnp.logical_not(from_me(j)))
        def _():
            remote(index_out.at[0], index_in.at[j], isend_sem.at[0], irecv_sem.at[j], 0).wait_recv()

        table = table_ref[...]
        for r in range(rows):
            ids = jnp.broadcast_to(index_in[j, pl.ds(r, 1), :], (levels, groups))
            hot = (ids == lax.broadcasted_iota(jnp.int32, (levels, groups), 0)).astype(jnp.float32)
            found = lax.dot_general(
                hot, table, (((0,), (0,)), ((), ())),
                precision=HIGHEST, preferred_element_type=jnp.float32,
            )
            scales_ref[r, pl.ds(pl.multiple_of(j * groups, groups), groups), :] = found

    @pl.loop(0, seqs)
    def _(j):
        @pl.when(jnp.logical_not(from_me(j)))
        def _():
            remote(sums.at[0], window(j), send_sem.at[0], recv_sem.at[j], 0).wait_recv()

    @pl.loop(0, blocks)
    def _(d):
        @pl.when(jnp.logical_not(is_me(d)))
        def _():
            send_index(d).wait_send()

            @pl.when(s == 0)
            def _():
                send_anchor(d).wait_send()

            send_sums(d).wait_send()

    @pl.loop(0, blocks // 2)
    def _(e):
        @pl.when(relayed(e))
        def _():
            for c in range(chunks):
                forward(e, c).wait_send()


def rebuild(sums_ref, scales_ref, base_ref, out_hbm, built, out_sem):
    many, length, channels = built.shape
    groups = scales_ref.shape[1]
    group_len = length // groups
    stores = [pltpu.make_async_copy(built.at[r], out_hbm.at[0, r], out_sem.at[r]) for r in range(many)]
    for r in range(many):

        def step(j, base, r=r):
            at = pl.multiple_of(j * group_len, group_len)
            x = sums_ref[r, pl.ds(at, group_len), :].astype(jnp.float32)
            grown = x * scales_ref[r, pl.ds(j, 1), :]
            built[r, pl.ds(at, group_len), :] = (grown + base).astype(jnp.bfloat16)
            return base + grown[group_len - 1:]

        lax.fori_loop(0, groups, step, base_ref[r], unroll=16)
        stores[r].start()
    for copy in stores:
        copy.wait()


def on_device(delta_codes, scale_index, anchor_codes, scale_table, anchor_scale):
    seqs, grps = lax.axis_size("seq"), lax.axis_size("grp")
    seq_local, kv_heads, tokens, channels = delta_codes.shape
    groups = scale_index.shape[2]
    heads = kv_heads // grps
    rows = seq_local * grps * heads // seqs
    blocks = seq_local * kv_heads // rows
    seq_rows, head_rows = max(1, rows // heads), min(rows, heads)
    chunks = min(rows, CHUNKS)
    length = seqs * tokens
    vmem = pl.BlockSpec(memory_space=pltpu.VMEM)
    hbm = pl.BlockSpec(memory_space=pltpu.HBM)
    sums, scales, base = pl.pallas_call(
        exchange,
        out_shape=(
            jax.ShapeDtypeStruct((rows, length, channels), jnp.bfloat16),
            jax.ShapeDtypeStruct((rows, seqs * groups, channels), jnp.float32),
            jax.ShapeDtypeStruct((rows, 1, channels), jnp.float32),
        ),
        in_specs=[hbm] * 5,
        out_specs=(vmem, vmem, vmem),
        scratch_shapes=[
            pltpu.VMEM((blocks, seq_rows, head_rows, tokens, channels), jnp.int32),
            pltpu.VMEM((blocks, rows, tokens, channels), jnp.bfloat16),
            pltpu.VMEM((blocks // 2, chunks, rows // chunks, tokens, channels), jnp.bfloat16),
            pltpu.VMEM((blocks, rows, groups), jnp.int32),
            pltpu.VMEM((seqs, rows, groups), jnp.int32),
            pltpu.VMEM((blocks, rows, channels), jnp.int32),
            pltpu.VMEM((rows, channels), jnp.int32),
            pltpu.SemaphoreType.DMA((blocks,)),
            pltpu.SemaphoreType.DMA((blocks,)),
            pltpu.SemaphoreType.DMA((seqs,)),
            pltpu.SemaphoreType.DMA((blocks,)),
            pltpu.SemaphoreType.DMA((seqs,)),
            pltpu.SemaphoreType.DMA((blocks,)),
            pltpu.SemaphoreType.DMA,
            pltpu.SemaphoreType.DMA((blocks // 2, chunks)),
            pltpu.SemaphoreType.DMA((blocks // 2,)),
            pltpu.VMEM(scale_index.shape, jnp.int32),
            pltpu.VMEM(anchor_codes.shape, jnp.int32),
            pltpu.VMEM(scale_table.shape, jnp.float32),
            pltpu.VMEM((1, channels), jnp.float32),
            pltpu.SemaphoreType.DMA((4,)),
        ],
        compiler_params=pltpu.CompilerParams(
            collective_id=0, has_side_effects=True, vmem_limit_bytes=48 * 1024 * 1024
        ),
        name="exchange",
    )(delta_codes, scale_index, anchor_codes, scale_table, anchor_scale[None])

    out = pl.pallas_call(
        rebuild,
        out_shape=jax.ShapeDtypeStruct((1, rows, length, channels), jnp.bfloat16),
        in_specs=[vmem] * 3,
        out_specs=hbm,
        scratch_shapes=[
            pltpu.VMEM(sums.shape, jnp.bfloat16),
            pltpu.SemaphoreType.DMA((rows,)),
        ],
        compiler_params=pltpu.CompilerParams(vmem_limit_bytes=16 * 1024 * 1024),
        name="rebuild",
    )(sums, scales, base)
    return out


def solution(mesh):
    placed = (P("grp", None, "seq", None), P("grp", None, "seq"), P("grp", None, None), P(), P())
    return jax.shard_map(
        on_device,
        mesh=mesh,
        in_specs=placed,
        out_specs=P("grp", "seq", None, None),
        check_vma=False,
    )
```
